32 devices in a mesh: section: 4 (over y, x), seq: 2 (over core), tensor: 4 (over z).
Axes of the slice: x: 2, y: 2, z: 4, core: 2. Of those that a mesh axis runs over, the one named last changes fastest.
Arguments:
- states_in: bfloat16 [1, 256, 4608], P(None, 'seq', 'tensor'), may hold values from -100 to 100
- span_order: int32 [4], replicated, may hold values from 0 to 3, each once
- pre_gain: bfloat16 [4, 4608], P('section'), may hold values from 0.25 to 1.75
- w_query: bfloat16 [4, 4608, 4096], P('section', None, 'tensor'), may hold values from -0.09375 to 0.09375
- w_key: bfloat16 [4, 4608, 2048], P('section', None, 'tensor'), may hold values from -0.09375 to 0.09375
- w_value: bfloat16 [4, 4608, 2048], P('section', None, 'tensor'), may hold values from -0.09375 to 0.09375
- w_out: bfloat16 [4, 4096, 4608], P('section', 'tensor'), may hold values from -0.125 to 0.125
- post_gain: bfloat16 [4, 4608], P('section'), may hold values from 0.25 to 1.75
Outputs:
- states: bfloat16 [4, 1, 256, 4608], P('section', None, 'seq', 'tensor')
The draws below stay inside these ranges and needn't reach their ends.
Inputs may be any that keep to these rules, and one draw needn't show every extreme that they name: Each span number appears once; row block j of 64 rows holds the tokens from position span_order[j] * 64 on.
All inputs are finite; a program needn't handle non-finite values.
Results may differ from the reference program's by a relative error of at most 0.024.
Values may be sent and summed in bfloat16 or wider, within the bound.
A program may use at most 128 MiB of HBM per device.

```python
import jax
import jax.numpy as jnp
from jax import lax

D = 4608
HEADS = 32
KV_HEADS = 16
HEAD_DIM = 128
MICRO = 1
LAYERS = 4
SEQLEN = 256
SPAN = 64
N_SEQ = 2
N_TENSOR = 4


def draw_states_in(key, part):
    shape_full = (MICRO, SEQLEN, D)
    key_base = jax.random.fold_in(key, 11)
    sample = jnp.clip(jax.random.normal(key_base, shape_full, jnp.float32), -4.0, 4.0)
    return sample.astype(jnp.bfloat16)


def spiked(entries, own_key, source, target, blocks, factor):
    owner, partner = [(jnp.arange(entries.shape[axis_at]) // (entries.shape[axis_at] // blocks)).reshape([-1 if axis == axis_at else 1 for axis in range(entries.ndim)]) for axis_at in (source, target)]
    chosen = jax.random.permutation(own_key, blocks)[partner]
    strong = (owner == chosen) | (owner == (partner + blocks // 2) % blocks)
    return jnp.where(strong, factor * entries, entries)


def level_of(rng, shape, cuts, low, high):
    def one(axis_at, shards_of):
        draws = jax.random.uniform(jax.random.fold_in(jax.random.fold_in(rng, 6), axis_at), (shards_of,), jnp.float32, low / len(cuts), high / len(cuts))
        return jnp.repeat(jnp.exp(draws), shape[axis_at] // shards_of).reshape((-1,) + (1,) * (len(shape) - axis_at - 1))

    factor_of = one(*cuts[0])
    for cut in cuts[1:]:
        factor_of = factor_of * one(*cut)
    return factor_of


def gaussian(stream_key, extent, deviation, reach, cuts=(), held_as=jnp.bfloat16):
    entries = jax.random.normal(stream_key, extent, jnp.float32) * deviation
    if len(cuts) > 0:
        entries = level_of(stream_key, extent, cuts, -0.22, 0.18) * entries
    return jnp.clip(entries, min=-reach, max=reach).astype(held_as)


def gaussian_with(rng, dims, deviation, reach, cuts, heavy, held_as=jnp.bfloat16):
    values = deviation * jax.random.normal(rng, dims, jnp.float32)
    if cuts:
        values = values * level_of(rng, dims, cuts, -0.22, 0.18)
    return jnp.clip(spiked(values, jax.random.fold_in(rng, 3), *heavy), -reach, reach).astype(held_as)


def setup_inputs(seed: int = 0) -> dict:
    splits = jax.random.split(jax.random.key(seed), 9)
    states_in = draw_states_in(jax.random.fold_in(splits[8], 71), 0)
    span_order = jax.random.permutation(splits[1], 2 * N_SEQ).astype(jnp.int32)
    pre_gain = jnp.clip(1.0 + 0.15 * jax.random.normal(splits[2], (LAYERS, D), jnp.float32), 0.25, 1.75).astype(jnp.bfloat16)
    w_query = gaussian(splits[3], (LAYERS, D, HEADS * HEAD_DIM), D ** -0.5, 0.09375, ((0, 4), (2, 4)))
    w_key = gaussian(splits[4], (LAYERS, D, KV_HEADS * HEAD_DIM), D ** -0.5, 0.09375, ((0, 4), (2, 4)))
    w_value = gaussian(splits[5], (LAYERS, D, KV_HEADS * HEAD_DIM), D ** -0.5, 0.09375, ((0, 4), (2, 4)))
    w_out = gaussian_with(splits[6], (LAYERS, HEADS * HEAD_DIM, D), (HEADS * HEAD_DIM) ** -0.5, 0.125, ((0, 4), (1, 4)), (1, 2, 4, 2.0))
    post_gain = jnp.clip(1.0 + 0.15 * jax.random.normal(splits[7], (LAYERS, D), jnp.float32), 0.25, 1.75).astype(jnp.bfloat16)
    return {"states_in": states_in, "span_order": span_order, "pre_gain": pre_gain, "w_query": w_query, "w_key": w_key, "w_value": w_value, "w_out": w_out, "post_gain": post_gain}


softcap_limit = 50.0
query_scale = 144.0 ** (-0.5)
epsilon = 1e-06
rotary_base = 10000.0

def rounded(array):
    return lax.optimization_barrier(array.astype(jnp.bfloat16)).astype(jnp.float32)

def rotate(vectors, places):
    half_dim = vectors.shape[-1] // 2
    inverse = rotary_base ** (-(jnp.arange(half_dim, dtype=jnp.float32) * 2.0 / vectors.shape[-1]))
    angles = places.astype(jnp.float32)[:, None] * inverse[None, :]
    cos_part = jnp.cos(angles)[:, None, :]
    sin_part = jnp.sin(angles)[:, None, :]
    lower_half = vectors[..., :half_dim]
    upper_half = vectors[..., half_dim:]
    return jnp.concatenate([lower_half * cos_part - upper_half * sin_part, upper_half * cos_part + lower_half * sin_part], axis=-1)

def one_layer(stream_in, places, allowed, gain_in, query_w, key_w, value_w, out_w, gain_out):
    group_size = HEADS // KV_HEADS
    local_heads = HEADS // N_TENSOR
    stream = stream_in.astype(jnp.float32)
    normed = (stream * lax.rsqrt(lax.optimization_barrier(jnp.mean(stream * stream, axis=1, keepdims=True)) + epsilon) * gain_in.astype(jnp.float32)).astype(jnp.bfloat16)
    queries = jnp.dot(normed, query_w, preferred_element_type=jnp.float32).reshape(SEQLEN, HEADS, HEAD_DIM)
    queries = rounded(rotate(queries, places) * query_scale).reshape(SEQLEN, KV_HEADS, group_size, HEAD_DIM)
    key_rows = jnp.dot(normed, key_w, preferred_element_type=jnp.float32).reshape(SEQLEN, KV_HEADS, HEAD_DIM)
    key_rows = rounded(rotate(key_rows, places))
    values = rounded(jnp.dot(normed, value_w, preferred_element_type=jnp.float32)).reshape(SEQLEN, KV_HEADS, HEAD_DIM)
    scores = jnp.einsum('tkgd,pkd->kgtp', queries, key_rows, precision=lax.Precision.HIGHEST)
    capped = softcap_limit * jnp.tanh(scores / softcap_limit)
    weight = jnp.where(allowed[None, None], jnp.exp(capped), jnp.float32(0.0))
    totals = lax.optimization_barrier(jnp.sum(weight, axis=3))
    numerator = jnp.einsum('kgtp,pkd->tkgd', rounded(weight), values, precision=lax.Precision.HIGHEST)
    attended = (numerator / jnp.transpose(totals, (2, 0, 1))[..., None]).astype(jnp.bfloat16)
    attended = attended.reshape(SEQLEN, N_TENSOR, local_heads * HEAD_DIM)
    out_groups = out_w.reshape(N_TENSOR, local_heads * HEAD_DIM, D)
    projected = jnp.zeros((SEQLEN, D), jnp.float32)
    for group_index in range(N_TENSOR):
        term = jnp.dot(attended[:, group_index], out_groups[group_index], preferred_element_type=jnp.float32)
        projected = projected + rounded(term)
    scaling = lax.rsqrt(lax.optimization_barrier(jnp.mean(projected * projected, axis=1, keepdims=True)) + epsilon)
    return (stream + projected * scaling * gain_out.astype(jnp.float32)).astype(jnp.bfloat16)

def reference(states_in, span_order, pre_gain, w_query, w_key, w_value, w_out, post_gain):
    row_ids = jnp.arange(SEQLEN, dtype=jnp.int32)
    places = (span_order[row_ids // SPAN] * SPAN + row_ids % SPAN).astype(jnp.int32)
    allowed = places[None, :] <= places[:, None]
    per_layer = []
    for layer_index in range(LAYERS):
        per_layer.append([])
    for micro_index in range(MICRO):
        stream = states_in[micro_index]
        for layer_index in range(LAYERS):
            stream = one_layer(stream, places, allowed, pre_gain[layer_index], w_query[layer_index], w_key[layer_index], w_value[layer_index], w_out[layer_index], post_gain[layer_index])
            per_layer[layer_index].append(stream)
    return jnp.stack([jnp.stack(items, axis=0) for items in per_layer], axis=0)
```

```python
import functools
import math

import jax
import jax.numpy as jnp
from jax import lax
from jax.experimental import pallas as pl
from jax.experimental.pallas import tpu as pltpu
from jax.sharding import PartitionSpec as P

HEAD_DIM = 128

softcap_limit = 50.0
query_scale = 144.0 ** (-0.5)
epsilon = 1e-06
rotary_base = 10000.0

MESH = pl.DeviceIdType.MESH
f32 = jnp.float32
bf16 = jnp.bfloat16


def kernel(
    sections, seqs, tensors,
    states, order, gain_in, wq_hbm, wk_hbm, wv_hbm, wo_hbm, gain_out, out,
    wq, wk, wv, wo, x, acc_q, acc_kv, kv, qh, att, part, from_left, from_right, total, fresh, landed,
    w_sem, x0_recv, x0_right, x0_left, x_recv, x_right, x_left, kv_send, kv_recv,
    l_recv, r_recv, l_send, r_send, next_send, out_send, out_recv,
):
    s = lax.axis_index("section")
    q = lax.axis_index("seq")
    z = lax.axis_index("tensor")
    _, rows, width = states.shape
    chunks = x.shape[0]
    model = chunks * width
    part_rows = rows // tensors
    q_width = wq.shape[1]
    kv_width = wk.shape[1]
    q_heads = q_width // HEAD_DIM
    kv_heads = kv_width // HEAD_DIM
    group = q_heads // kv_heads
    span_count = order.shape[0]
    span = rows * seqs // span_count

    def remote(src, dst, send, recv, device):
        return pltpu.make_async_remote_copy(
            src_ref=src, dst_ref=dst, send_sem=send, recv_sem=recv, device_id=device, device_id_type=MESH
        )

    right = {"tensor": lax.rem(z + 1, tensors)}
    left = {"tensor": lax.rem(z + tensors - 1, tensors)}
    after = {"section": lax.rem(s + 1, sections)}

    loads = [
        pltpu.make_async_copy(src.at[0], dst, w_sem.at[i])
        for i, (src, dst) in enumerate(((wk_hbm, wk), (wv_hbm, wv), (wq_hbm, wq), (wo_hbm, wo)))
    ]
    for load in loads:
        load.start()

    barrier = pltpu.get_barrier_semaphore()
    for step in range(1, tensors):
        pl.semaphore_signal(barrier, inc=1, device_id={"tensor": lax.rem(z + step, tensors)}, device_id_type=MESH)
    for step in range(1, seqs):
        pl.semaphore_signal(barrier, inc=1, device_id={"seq": lax.rem(q + step, seqs)}, device_id_type=MESH)
    pl.semaphore_signal(barrier, inc=1, device_id=after, device_id_type=MESH)
    pl.semaphore_signal(barrier, inc=1, device_id={"section": lax.rem(s + sections - 1, sections)}, device_id_type=MESH)
    pl.semaphore_wait(barrier, tensors - 1 + seqs - 1 + 2)

    def block(o):
        return pl.ds(pl.multiple_of(o * part_rows, part_rows), part_rows)

    def first_right(o, src):
        return remote(src, x.at[o], x0_right.at[o], x0_recv.at[o], right)

    def first_left(o, src):
        return remote(src, x.at[o], x0_left.at[o], x0_recv.at[o], left)

    @pl.when(s == 0)
    def _():
        @pl.when(z < tensors - 1)
        def _():
            first_right(z, states.at[0]).start()

        @pl.when(z > 0)
        def _():
            first_left(z, states.at[0]).start()

        x[z] = states[0]

    row = lax.broadcasted_iota(jnp.int32, (rows, HEAD_DIM), 0) + q * rows
    starts = jnp.zeros((rows, HEAD_DIM), jnp.int32)
    key_col = lax.broadcasted_iota(jnp.int32, (1, rows * seqs), 1)
    key_starts = jnp.zeros((1, rows * seqs), jnp.int32)
    for j in range(span_count):
        begin = order[j] * span
        starts = jnp.where(row // span == j, begin, starts)
        key_starts = jnp.where(key_col // span == j, begin, key_starts)
    places = starts + row % span
    key_places = key_starts + key_col % span
    half = HEAD_DIM // 2
    lane = lax.broadcasted_iota(jnp.int32, (rows, HEAD_DIM), 1)
    inverse = jnp.exp((lane % half).astype(f32) * (-2.0 / HEAD_DIM * math.log(rotary_base)))
    angles = places.astype(f32) * inverse
    cos = jnp.cos(angles)
    sin = jnp.sin(angles) * jnp.where(lane < half, -1.0, 1.0)

    def rope(u):
        return u * cos + pltpu.roll(u, half, 1) * sin

    @pl.when(s == 0)
    def _():
        for d in range(1, tensors):
            @pl.when(z >= d)
            def _():
                first_right(z - d, x.at[z - d]).wait_recv()

                @pl.when(z < tensors - 1)
                def _():
                    first_right(z - d, x.at[z - d]).start()

            @pl.when(z + d < tensors)
            def _():
                first_left(z + d, x.at[z + d]).wait_recv()

                @pl.when(z > 0)
                def _():
                    first_left(z + d, x.at[z + d]).start()

    def piece(c, o, send, device):
        ref = x.at[c, block(o)]
        return remote(ref, ref, send.at[c, o], x_recv.at[c, o], device)

    acc_q[...] = jnp.zeros_like(acc_q)
    acc_kv[...] = jnp.zeros_like(acc_kv)
    for load in loads[:3]:
        load.wait()

    def finish_kv(scale):
        for k in range(kv_heads):
            cols = pl.ds(k * HEAD_DIM, HEAD_DIM)
            kv[q, :, cols] = rope(acc_kv[:, cols] * scale).astype(bf16)
        kv[q, :, kv_width:] = (acc_kv[:, kv_width:] * scale).astype(bf16)

    def take_chunk(c, squares):
        @pl.when(s > 0)
        def _():
            for d in range(tensors):
                if d == 0:
                    piece(c, z, x_right, right).wait_recv()

                    @pl.when(z < tensors - 1)
                    def _():
                        piece(c, z, x_right, right).start()

                    @pl.when(z > 0)
                    def _():
                        piece(c, z, x_left, left).start()
                else:
                    @pl.when(z >= d)
                    def _():
                        piece(c, z - d, x_right, right).wait_recv()

                        @pl.when(z < tensors - 1)
                        def _():
                            piece(c, z - d, x_right, right).start()

                    @pl.when(z + d < tensors)
                    def _():
                        piece(c, z + d, x_left, left).wait_recv()

                        @pl.when(z > 0)
                        def _():
                            piece(c, z + d, x_left, left).start()

        stream = x[c].astype(f32)
        squares = squares + jnp.sum(stream * stream, axis=1, keepdims=True)
        scaled = (stream * gain_in[c].astype(f32)).astype(bf16)
        depth = pl.ds(pl.multiple_of(c * width, width), width)
        acc_kv[:, :kv_width] += jnp.dot(scaled, wk[depth, :], preferred_element_type=f32)
        acc_kv[:, kv_width:] += jnp.dot(scaled, wv[depth, :], preferred_element_type=f32)
        acc_q[...] += jnp.dot(scaled, wq[depth, :], preferred_element_type=f32)
        return squares

    squares = lax.fori_loop(0, chunks, take_chunk, jnp.zeros((rows, 1), f32))
    scale = lax.rsqrt(squares / model + epsilon)
    finish_kv(scale)

    def kv_copy(j, device):
        return remote(kv.at[j], kv.at[j], kv_send.at[device], kv_recv.at[j], {"seq": device})

    for step in range(1, seqs):
        kv_copy(q, lax.rem(q + step, seqs)).start()
    for h in range(q_heads):
        cols = pl.ds(h * HEAD_DIM, HEAD_DIM)
        qh[:, cols] = (rope(acc_q[:, cols] * scale) * query_scale).astype(bf16)
    for step in range(1, seqs):
        other = lax.rem(q + step, seqs)
        kv_copy(other, other).wait_recv()

    dims = (((1,), (1,)), ((), ()))
    for h in range(q_heads):
        k = h // group
        cols = pl.ds(h * HEAD_DIM, HEAD_DIM)
        queries = qh[:, cols]
        numerator = jnp.zeros((rows, HEAD_DIM), f32)
        totals = jnp.zeros((rows, 1), f32)
        for j in range(seqs):
            keys = kv[j, :, k * HEAD_DIM:(k + 1) * HEAD_DIM]
            vals = kv[j, :, kv_width + k * HEAD_DIM:kv_width + (k + 1) * HEAD_DIM]
            scores = lax.dot_general(queries, keys, dims, preferred_element_type=f32)
            capped = softcap_limit * jnp.tanh(scores * (1.0 / softcap_limit))
            allowed = key_places[:, j * rows:(j + 1) * rows] <= places[:, :1]
            weight = jnp.where(allowed, jnp.exp(capped), 0.0)
            totals = totals + jnp.sum(weight, axis=1, keepdims=True)
            numerator = numerator + jnp.dot(weight.astype(bf16), vals, preferred_element_type=f32)
        att[:, cols] = (numerator / totals).astype(bf16)

    loads[3].wait()

    def chain_right(c, b, src):
        return remote(src, from_left.at[c, b], r_send.at[c, b], l_recv.at[c, b], right)

    def chain_left(c, b, src):
        return remote(src, from_right.at[c, b], l_send.at[c, b], r_recv.at[c, b], left)

    def project(c, carry):
        cols = pl.ds(c * width if isinstance(c, int) else pl.multiple_of(c * width, width), width)
        part[c] = jnp.dot(att[...], wo[:, cols], preferred_element_type=f32).astype(bf16)
        for k in range(tensors):
            far = tensors - 1 - k

            @pl.when(jnp.logical_and(z == 0, far > 0))
            def _():
                chain_right(c, far, part.at[c, block(far)]).start()

            @pl.when(jnp.logical_and(z == tensors - 1, k < tensors - 1))
            def _():
                chain_left(c, k, part.at[c, block(k)]).start()

            @pl.when(jnp.logical_and(z > 0, far > z))
            def _():
                chain_right(c, far, from_left.at[c, far]).wait_recv()
                from_left[c, far] = (from_left[c, far].astype(f32) + part[c, block(far)].astype(f32)).astype(bf16)
                chain_right(c, far, from_left.at[c, far]).start()

            @pl.when(jnp.logical_and(z < tensors - 1, k < z))
            def _():
                chain_left(c, k, from_right.at[c, k]).wait_recv()
                from_right[c, k] = (from_right[c, k].astype(f32) + part[c, block(k)].astype(f32)).astype(bf16)
                chain_left(c, k, from_right.at[c, k]).start()
        return carry

    if width % 128 == 0:
        lax.fori_loop(0, chunks, project, 0)
    else:
        for c in range(chunks):
            project(c, 0)

    own = block(z)

    def gather_sum(c, squares):
        total[c] = part[c, own].astype(f32)

        @pl.when(z > 0)
        def _():
            chain_right(c, z, from_left.at[c, z]).wait_recv()
            total[c] += from_left[c, z].astype(f32)

        @pl.when(z < tensors - 1)
        def _():
            chain_left(c, z, from_right.at[c, z]).wait_recv()
            total[c] += from_right[c, z].astype(f32)

        value = total[c]
        return squares + jnp.sum(value * value, axis=1, keepdims=True)

    squares = lax.fori_loop(0, chunks, gather_sum, jnp.zeros((part_rows, 1), f32))
    scaling = lax.rsqrt(squares / model + epsilon)

    def onward(c):
        return remote(fresh.at[c], x.at[c, own], next_send.at[c], x_recv.at[c, z], after)

    def share(c):
        return remote(fresh.at[c], landed.at[own], out_send.at[c], out_recv.at[z], {"tensor": c})

    for c in range(chunks):
        fresh[c] = (x[c, own].astype(f32) + total[c] * scaling * gain_out[c].astype(f32)).astype(bf16)

        @pl.when(s < sections - 1)
        def _():
            onward(c).start()

    for c in range(chunks):
        @pl.when(z != c)
        def _():
            share(c).start()

    landed[own] = fresh[z]
    for o in range(tensors):
        @pl.when(z != o)
        def _():
            remote(fresh.at[o], landed.at[block(o)], out_send.at[o], out_recv.at[o], {"tensor": o}).wait_recv()
    out[0, 0] = landed[...]

    for c in range(chunks):
        @pl.when(s < sections - 1)
        def _():
            onward(c).wait_send()

        @pl.when(z != c)
        def _():
            share(c).wait_send()

    for step in range(1, seqs):
        kv_copy(q, lax.rem(q + step, seqs)).wait_send()

    for o in range(tensors):
        @pl.when(jnp.logical_and(s == 0, jnp.logical_and(z < tensors - 1, o <= z)))
        def _():
            first_right(o, x.at[o]).wait_send()

        @pl.when(jnp.logical_and(s == 0, jnp.logical_and(z > 0, o >= z)))
        def _():
            first_left(o, x.at[o]).wait_send()

    def drain(c, carry):
        for o in range(tensors):
            @pl.when(jnp.logical_and(s > 0, jnp.logical_and(z < tensors - 1, o <= z)))
            def _():
                piece(c, o, x_right, right).wait_send()

            @pl.when(jnp.logical_and(s > 0, jnp.logical_and(z > 0, o >= z)))
            def _():
                piece(c, o, x_left, left).wait_send()

            @pl.when(o > z)
            def _():
                chain_right(c, o, from_left.at[c, o]).wait_send()

            @pl.when(o < z)
            def _():
                chain_left(c, o, from_right.at[c, o]).wait_send()
        return carry

    lax.fori_loop(0, chunks, drain, 0)


def body(sections, seqs, tensors, states_in, span_order, pre_gain, w_query, w_key, w_value, w_out, post_gain):
    _, rows, width = states_in.shape
    model = pre_gain.shape[1]
    chunks = model // width
    part_rows = rows // tensors
    q_width, kv_width = w_query.shape[2], w_key.shape[2]
    vmem = pl.BlockSpec(memory_space=pltpu.VMEM)
    hbm = pl.BlockSpec(memory_space=pl.ANY)
    smem = pl.BlockSpec(memory_space=pltpu.SMEM)
    dma = pltpu.SemaphoreType.DMA
    grid2 = (chunks, tensors)
    return pl.pallas_call(
        functools.partial(kernel, sections, seqs, tensors),
        out_shape=jax.ShapeDtypeStruct((1, 1, rows, width), bf16),
        in_specs=[vmem, smem, vmem, hbm, hbm, hbm, hbm, vmem],
        out_specs=vmem,
        scratch_shapes=[
            pltpu.VMEM((model, q_width), bf16),
            pltpu.VMEM((model, kv_width), bf16),
            pltpu.VMEM((model, kv_width), bf16),
            pltpu.VMEM((q_width, model), bf16),
            pltpu.VMEM((chunks, rows, width), bf16),
            pltpu.VMEM((rows, q_width), f32),
            pltpu.VMEM((rows, 2 * kv_width), f32),
            pltpu.VMEM((seqs, rows, 2 * kv_width), bf16),
            pltpu.VMEM((rows, q_width), bf16),
            pltpu.VMEM((rows, q_width), bf16),
            pltpu.VMEM((chunks, rows, width), bf16),
            pltpu.VMEM((chunks, tensors, part_rows, width), bf16),
            pltpu.VMEM((chunks, tensors, part_rows, width), bf16),
            pltpu.VMEM((chunks, part_rows, width), f32),
            pltpu.VMEM((chunks, part_rows, width), bf16),
            pltpu.VMEM((rows, width), bf16),
            dma((4,)),
            dma((tensors,)), dma((tensors,)), dma((tensors,)),
            dma(grid2), dma(grid2), dma(grid2),
            dma((seqs,)), dma((seqs,)),
            dma(grid2), dma(grid2), dma(grid2), dma(grid2),
            dma((chunks,)), dma((tensors,)), dma((tensors,)),
        ],
        compiler_params=pltpu.CompilerParams(
            collective_id=0, has_side_effects=True, vmem_limit_bytes=60 * 1024 * 1024
        ),
    )(
        states_in, span_order, pre_gain.reshape(chunks, 1, width), w_query, w_key, w_value, w_out,
        post_gain.reshape(chunks, 1, width),
    )


def solution(mesh):
    in_specs = (
        P(None, "seq", "tensor"),
        P(),
        P("section", None),
        P("section", None, "tensor"),
        P("section", None, "tensor"),
        P("section", None, "tensor"),
        P("section", "tensor", None),
        P("section", None),
    )
    out_specs = P("section", None, "seq", "tensor")
    sizes = (mesh.shape["section"], mesh.shape["seq"], mesh.shape["tensor"])
    return jax.shard_map(
        functools.partial(body, *sizes), mesh=mesh, in_specs=in_specs, out_specs=out_specs, check_vma=False
    )
```

```python
import functools
import math

import jax
import jax.numpy as jnp
from jax import lax
from jax.experimental import pallas as pl
from jax.experimental.pallas import tpu as pltpu
from jax.sharding import PartitionSpec as P

HEAD_DIM = 128

softcap_limit = 50.0
query_scale = 144.0 ** (-0.5)
epsilon = 1e-06
rotary_base = 10000.0

MESH = pl.DeviceIdType.MESH
f32 = jnp.float32
bf16 = jnp.bfloat16


def kernel(
    sections, seqs, tensors,
    states, order, gain_in, wq_hbm, wk_hbm, wv_hbm, wo_hbm, gain_out, out,
    wq, wk, wv, wo, x, acc_q, acc_kv, kv, qh, att, part, from_left, from_right, total, fresh, landed,
    relay, raw, back, cos_ref, sin_ref,
    w_sem, x_recv, x_right, x_left, relay_recv, deliver_send, kv_send, kv_recv,
    l_recv, r_recv, l_send, r_send, raw_send, raw_recv, back_send, back_recv, next_send, out_send, out_recv,
):
    t = lax.axis_index("section")
    q = lax.axis_index("seq")
    z = lax.axis_index("tensor")
    _, rows, width = states.shape
    chunks = x.shape[0]
    model = chunks * width
    part_rows = rows // tensors
    q_width = wq.shape[1]
    kv_width = wk.shape[1]
    q_heads = q_width // HEAD_DIM
    kv_heads = kv_width // HEAD_DIM
    group = q_heads // kv_heads
    span_count = order.shape[0]
    span = rows * seqs // span_count
    roles = 2

    def helper(s, r):
        return s + 1 - 2 * lax.rem(s, 2) if r == 0 else lax.rem(s + sections // 2, sections)

    def remote(src, dst, send, recv, device):
        return pltpu.make_async_remote_copy(
            src_ref=src, dst_ref=dst, send_sem=send, recv_sem=recv, device_id=device, device_id_type=MESH
        )

    right = {"tensor": lax.rem(z + 1, tensors)}
    left = {"tensor": lax.rem(z + tensors - 1, tensors)}

    loads = [
        pltpu.make_async_copy(src.at[0], dst, w_sem.at[i])
        for i, (src, dst) in enumerate(((wk_hbm, wk), (wv_hbm, wv), (wq_hbm, wq), (wo_hbm, wo)))
    ]
    for load in loads:
        load.start()

    barrier = pltpu.get_barrier_semaphore()
    for axis, here, count in (("tensor", z, tensors), ("seq", q, seqs), ("section", t, sections)):
        for step in range(1, count):
            pl.semaphore_signal(barrier, inc=1, device_id={axis: lax.rem(here + step, count)}, device_id_type=MESH)
    pl.semaphore_wait(barrier, tensors + seqs + sections - 3)

    def block(o):
        return pl.ds(pl.multiple_of(o * part_rows, part_rows), part_rows)

    def piece(s, c, o):
        first = 1 - lax.div(s + sections - 1, sections)
        return x.at[c + first * (o - c), block(o + first * (c - o))]

    def gather(cs, ref, recv, ready, arrived):
        for d in range(tensors):
            for c in cs:
                def step(o, go_right, go_left):
                    if go_right:
                        @pl.when(z < tensors - 1)
                        def _():
                            remote(ref(c, o), ref(c, o), x_right.at[c, o], recv.at[c, o], right).start()
                    if go_left:
                        @pl.when(z > 0)
                        def _():
                            remote(ref(c, o), ref(c, o), x_left.at[c, o], recv.at[c, o], left).start()

                if d == 0:
                    ready(c)
                    step(z, True, True)
                    arrived(z)
                else:
                    @pl.when(z >= d)
                    def _():
                        remote(ref(c, z - d), ref(c, z - d), x_right.at[c, z - d], recv.at[c, z - d], right).wait_recv()
                        step(z - d, True, False)
                        arrived(z - d)

                    @pl.when(z + d < tensors)
                    def _():
                        remote(ref(c, z + d), ref(c, z + d), x_left.at[c, z + d], recv.at[c, z + d], left).wait_recv()
                        step(z + d, False, True)
                        arrived(z + d)

    def chain_right(c, b, src):
        return remote(src, from_left.at[c, b], r_send.at[c, b], l_recv.at[c, b], right)

    def chain_left(c, b, src):
        return remote(src, from_right.at[c, b], l_send.at[c, b], r_recv.at[c, b], left)

    def chain(cs, mine):
        for k in range(tensors):
            far = tensors - 1 - k
            for c in cs:
                @pl.when(jnp.logical_and(z == 0, far > 0))
                def _():
                    chain_right(c, far, mine(c, far)).start()

                @pl.when(jnp.logical_and(z == tensors - 1, k < tensors - 1))
                def _():
                    chain_left(c, k, mine(c, k)).start()

                @pl.when(jnp.logical_and(z > 0, far > z))
                def _():
                    chain_right(c, far, from_left.at[c, far]).wait_recv()
                    from_left[c, far] = (from_left[c, far].astype(f32) + mine(c, far)[...].astype(f32)).astype(bf16)
                    chain_right(c, far, from_left.at[c, far]).start()

                @pl.when(jnp.logical_and(z < tensors - 1, k < z))
                def _():
                    chain_left(c, k, from_right.at[c, k]).wait_recv()
                    from_right[c, k] = (from_right[c, k].astype(f32) + mine(c, k)[...].astype(f32)).astype(bf16)
                    chain_left(c, k, from_right.at[c, k]).start()

    def chain_end(c, mine):
        total[c] = mine(c, z)[...].astype(f32)

        @pl.when(z > 0)
        def _():
            chain_right(c, z, from_left.at[c, z]).wait_recv()
            total[c] += from_left[c, z].astype(f32)

        @pl.when(z < tensors - 1)
        def _():
            chain_left(c, z, from_right.at[c, z]).wait_recv()
            total[c] += from_right[c, z].astype(f32)

    def relay_ref(c, o):
        return relay.at[c, o]

    def deliver(s, r, o):
        return remote(relay.at[r, o], piece(s, r, o), deliver_send.at[r, o], x_recv.at[r, o], {"section": s})

    def onward_relay(r):
        goal = lax.rem(t + 1, sections)
        return remote(fresh.at[r], relay.at[r, z], next_send.at[r], relay_recv.at[r, z], {"section": helper(goal, r)})

    def onward(c):
        goal = lax.rem(t + 1, sections)
        return remote(fresh.at[c], x.at[c, block(z)], next_send.at[c], x_recv.at[c, z], {"section": goal})

    def raw_copy(r):
        return remote(part.at[r], raw.at[r], raw_send.at[r], raw_recv.at[r], {"section": helper(t, r)})

    def back_copy(r):
        return remote(relay.at[roles + r, 0], back.at[r], back_send.at[r], back_recv.at[r], {"section": helper(t, r)})

    def raw_block(c, b):
        return raw.at[c, block(b)]

    def help_gather(s, r):
        def ready(c):
            @pl.when(s == 0)
            def _():
                relay[r, z] = states[0, r * part_rows:(r + 1) * part_rows, :]

            @pl.when(jnp.logical_and(s > 0, s == t + 1))
            def _():
                relay[r, z] = fresh[r]

            @pl.when(jnp.logical_and(s > 0, s != t + 1))
            def _():
                onward_relay(r).wait_recv()

        gather([r], relay_ref, relay_recv, ready, lambda o: deliver(s, r, o).start())

    def help_reduce(r):
        raw_copy(r).wait_recv()
        chain([r], raw_block)
        chain_end(r, raw_block)
        relay[roles + r, 0] = total[r].astype(bf16)
        back_copy(r).start()

    half = HEAD_DIM // 2

    def positions():
        row = lax.broadcasted_iota(jnp.int32, (rows, HEAD_DIM), 0) + q * rows
        starts = jnp.zeros((rows, HEAD_DIM), jnp.int32)
        key_col = lax.broadcasted_iota(jnp.int32, (1, rows * seqs), 1)
        key_starts = jnp.zeros((1, rows * seqs), jnp.int32)
        for j in range(span_count):
            begin = order[j] * span
            starts = jnp.where(row // span == j, begin, starts)
            key_starts = jnp.where(key_col // span == j, begin, key_starts)
        return starts + row % span, key_starts + key_col % span

    def rope(u):
        return u * cos_ref[...] + pltpu.roll(u, half, 1) * sin_ref[...]

    def tables():
        places, _ = positions()
        lane = lax.broadcasted_iota(jnp.int32, (rows, HEAD_DIM), 1)
        inverse = jnp.exp((lane % half).astype(f32) * (-2.0 / HEAD_DIM * math.log(rotary_base)))
        angles = places.astype(f32) * inverse
        cos_ref[...] = jnp.cos(angles)
        sin_ref[...] = jnp.sin(angles) * jnp.where(lane < half, -1.0, 1.0)

    def kv_copy(j, device):
        return remote(kv.at[j], kv.at[j], kv_send.at[device], kv_recv.at[j], {"seq": device})

    def share(c):
        return remote(fresh.at[c], landed.at[block(z)], out_send.at[c], out_recv.at[z], {"tensor": c})

    def part_block(c, b):
        return part.at[c, block(b)]

    def layer():
        line = list(range(roles, chunks))

        def own_piece(c, o):
            return piece(t, c, o)

        def ready(c):
            @pl.when(t > 0)
            def _():
                onward(c).wait_recv()

        gather(line, own_piece, x_recv, ready, lambda o: None)
        for r in range(roles):
            for o in range(tensors):
                deliver(t, r, o).wait_recv()

        acc_q[...] = jnp.zeros_like(acc_q)
        acc_kv[...] = jnp.zeros_like(acc_kv)
        for load in loads[:3]:
            load.wait()

        def take_chunk(c, squares):
            stream = x[c].astype(f32)
            squares = squares + jnp.sum(stream * stream, axis=1, keepdims=True)
            scaled = (stream * gain_in[c].astype(f32)).astype(bf16)
            depth = pl.ds(pl.multiple_of(c * width, width), width)
            acc_kv[:, :kv_width] += jnp.dot(scaled, wk[depth, :], preferred_element_type=f32)
            acc_kv[:, kv_width:] += jnp.dot(scaled, wv[depth, :], preferred_element_type=f32)
            acc_q[...] += jnp.dot(scaled, wq[depth, :], preferred_element_type=f32)
            return squares

        squares = lax.fori_loop(0, chunks, take_chunk, jnp.zeros((rows, 1), f32))
        scale = lax.rsqrt(squares / model + epsilon)
        for k in range(kv_heads):
            cols = pl.ds(k * HEAD_DIM, HEAD_DIM)
            kv[q, :, cols] = rope(acc_kv[:, cols] * scale).astype(bf16)
        kv[q, :, kv_width:] = (acc_kv[:, kv_width:] * scale).astype(bf16)
        for step in range(1, seqs):
            kv_copy(q, lax.rem(q + step, seqs)).start()
        for h in range(q_heads):
            cols = pl.ds(h * HEAD_DIM, HEAD_DIM)
            qh[:, cols] = (rope(acc_q[:, cols] * scale) * query_scale).astype(bf16)
        for step in range(1, seqs):
            other = lax.rem(q + step, seqs)
            kv_copy(other, other).wait_recv()

        places, key_places = positions()
        dims = (((1,), (1,)), ((), ()))
        for h in range(q_heads):
            k = h // group
            cols = pl.ds(h * HEAD_DIM, HEAD_DIM)
            queries = qh[:, cols]
            numerator = jnp.zeros((rows, HEAD_DIM), f32)
            totals = jnp.zeros((rows, 1), f32)
            for j in range(seqs):
                keys = kv[j, :, k * HEAD_DIM:(k + 1) * HEAD_DIM]
                vals = kv[j, :, kv_width + k * HEAD_DIM:kv_width + (k + 1) * HEAD_DIM]
                scores = lax.dot_general(queries, keys, dims, preferred_element_type=f32)
                capped = softcap_limit * jnp.tanh(scores * (1.0 / softcap_limit))
                allowed = key_places[:, j * rows:(j + 1) * rows] <= places[:, :1]
                weight = jnp.where(allowed, jnp.exp(capped), 0.0)
                totals = totals + jnp.sum(weight, axis=1, keepdims=True)
                numerator = numerator + jnp.dot(weight.astype(bf16), vals, preferred_element_type=f32)
            att[:, cols] = (numerator / totals).astype(bf16)

        loads[3].wait()
        for c in range(chunks):
            part[c] = jnp.dot(
                att[...], wo[:, c * width:(c + 1) * width], preferred_element_type=f32
            ).astype(bf16)
            if c < roles:
                raw_copy(c).start()
        chain(line, part_block)
        for c in line:
            chain_end(c, part_block)
        squares = jnp.zeros((part_rows, 1), f32)
        for r in range(roles):
            back_copy(r).wait_recv()
            total[r] = back[r].astype(f32)
        for c in range(chunks):
            squares = squares + jnp.sum(total[c] * total[c], axis=1, keepdims=True)
        scaling = lax.rsqrt(squares / model + epsilon)
        for c in range(chunks):
            fresh[c] = (x[c, block(z)].astype(f32) + total[c] * scaling * gain_out[c].astype(f32)).astype(bf16)
            if c < roles:
                @pl.when(jnp.logical_and(t < sections - 1, helper(lax.rem(t + 1, sections), c) != t))
                def _():
                    onward_relay(c).start()
            else:
                @pl.when(t < sections - 1)
                def _():
                    onward(c).start()
        for c in range(chunks):
            @pl.when(z != c)
            def _():
                share(c).start()

    @pl.when(t == 0)
    def _():
        x[z, roles * part_rows:, :] = states[0, roles * part_rows:, :]

    tables()

    def turn(s, carry):
        @pl.when(s == t)
        def _():
            layer()

        for r in range(roles):
            @pl.when(s == helper(t, r))
            def _():
                help_gather(s, r)
                help_reduce(r)
        return carry

    lax.fori_loop(0, sections, turn, 0)

    own = block(z)
    landed[own] = fresh[z]
    for o in range(tensors):
        @pl.when(z != o)
        def _():
            remote(fresh.at[o], landed.at[block(o)], out_send.at[o], out_recv.at[o], {"tensor": o}).wait_recv()
    out[0, 0] = landed[...]

    for c in range(chunks):
        if c < roles:
            @pl.when(jnp.logical_and(t < sections - 1, helper(lax.rem(t + 1, sections), c) != t))
            def _():
                onward_relay(c).wait_send()
            raw_copy(c).wait_send()
            back_copy(c).wait_send()
            for o in range(tensors):
                deliver(helper(t, c), c, o).wait_send()
        else:
            @pl.when(t < sections - 1)
            def _():
                onward(c).wait_send()

        @pl.when(z != c)
        def _():
            share(c).wait_send()

    for step in range(1, seqs):
        kv_copy(q, lax.rem(q + step, seqs)).wait_send()

    def drain(c, carry):
        for o in range(tensors):
            @pl.when(jnp.logical_and(z < tensors - 1, o <= z))
            def _():
                remote(relay.at[0, o], relay.at[0, o], x_right.at[c, o], x_recv.at[c, o], right).wait_send()

            @pl.when(jnp.logical_and(z > 0, o >= z))
            def _():
                remote(relay.at[0, o], relay.at[0, o], x_left.at[c, o], x_recv.at[c, o], left).wait_send()

            @pl.when(o > z)
            def _():
                chain_right(c, o, from_left.at[c, o]).wait_send()

            @pl.when(o < z)
            def _():
                chain_left(c, o, from_right.at[c, o]).wait_send()
        return carry

    lax.fori_loop(0, chunks, drain, 0)


def body(sections, seqs, tensors, states_in, span_order, pre_gain, w_query, w_key, w_value, w_out, post_gain):
    _, rows, width = states_in.shape
    model = pre_gain.shape[1]
    chunks = model // width
    part_rows = rows // tensors
    q_width, kv_width = w_query.shape[2], w_key.shape[2]
    vmem = pl.BlockSpec(memory_space=pltpu.VMEM)
    hbm = pl.BlockSpec(memory_space=pl.ANY)
    smem = pl.BlockSpec(memory_space=pltpu.SMEM)
    dma = pltpu.SemaphoreType.DMA
    grid2 = (chunks, tensors)
    return pl.pallas_call(
        functools.partial(kernel, sections, seqs, tensors),
        out_shape=jax.ShapeDtypeStruct((1, 1, rows, width), bf16),
        in_specs=[vmem, smem, vmem, hbm, hbm, hbm, hbm, vmem],
        out_specs=vmem,
        scratch_shapes=[
            pltpu.VMEM((model, q_width), bf16),
            pltpu.VMEM((model, kv_width), bf16),
            pltpu.VMEM((model, kv_width), bf16),
            pltpu.VMEM((q_width, model), bf16),
            pltpu.VMEM((chunks, rows, width), bf16),
            pltpu.VMEM((rows, q_width), f32),
            pltpu.VMEM((rows, 2 * kv_width), f32),
            pltpu.VMEM((seqs, rows, 2 * kv_width), bf16),
            pltpu.VMEM((rows, q_width), bf16),
            pltpu.VMEM((rows, q_width), bf16),
            pltpu.VMEM((chunks, rows, width), bf16),
            pltpu.VMEM((chunks, tensors, part_rows, width), bf16),
            pltpu.VMEM((chunks, tensors, part_rows, width), bf16),
            pltpu.VMEM((chunks, part_rows, width), f32),
            pltpu.VMEM((chunks, part_rows, width), bf16),
            pltpu.VMEM((rows, width), bf16),
            pltpu.VMEM((4, tensors, part_rows, width), bf16),
            pltpu.VMEM((2, rows, width), bf16),
            pltpu.VMEM((2, part_rows, width), bf16),
            pltpu.VMEM((rows, HEAD_DIM), f32),
            pltpu.VMEM((rows, HEAD_DIM), f32),
            dma((4,)),
            dma(grid2), dma(grid2), dma(grid2),
            dma((2, tensors)), dma((2, tensors)),
            dma((seqs,)), dma((seqs,)),
            dma(grid2), dma(grid2), dma(grid2), dma(grid2),
            dma((2,)), dma((2,)), dma((2,)), dma((2,)),
            dma((chunks,)), dma((tensors,)), dma((tensors,)),
        ],
        compiler_params=pltpu.CompilerParams(
            collective_id=0, has_side_effects=True, vmem_limit_bytes=60 * 1024 * 1024
        ),
    )(
        states_in, span_order, pre_gain.reshape(chunks, 1, width), w_query, w_key, w_value, w_out,
        post_gain.reshape(chunks, 1, width),
    )


def solution(mesh):
    in_specs = (
        P(None, "seq", "tensor"),
        P(),
        P("section", None),
        P("section", None, "tensor"),
        P("section", None, "tensor"),
        P("section", None, "tensor"),
        P("section", "tensor", None),
        P("section", None),
    )
    out_specs = P("section", None, "seq", "tensor")
    sizes = (mesh.shape["section"], mesh.shape["seq"], mesh.shape["tensor"])
    return jax.shard_map(
        functools.partial(body, *sizes), mesh=mesh, in_specs=in_specs, out_specs=out_specs, check_vma=False
    )
```

```python
import functools
import math

import jax
import jax.numpy as jnp
from jax import lax
from jax.experimental import pallas as pl
from jax.experimental.pallas import tpu as pltpu
from jax.sharding import PartitionSpec as P

HEAD_DIM = 128

softcap_limit = 50.0
query_scale = 144.0 ** (-0.5)
epsilon = 1e-06
rotary_base = 10000.0

MESH = pl.DeviceIdType.MESH
f32 = jnp.float32
bf16 = jnp.bfloat16


def kernel(
    sections, seqs, tensors,
    states, order, gain_in, wq_hbm, wk_hbm, wv_hbm, wo_hbm, gain_out, out,
    wq, wk, wv, wo, x, acc_q, acc_kv, kv, qh, att, part, from_left, from_right, total, fresh, landed,
    relay, raw, back, cos_ref, sin_ref,
    w_sem, x_recv, x_right, x_left, relay_recv, deliver_send, kv_send, kv_recv,
    l_recv, r_recv, l_send, r_send, raw_send, raw_recv, back_send, back_recv, next_send, out_send, out_recv,
):
    t = lax.axis_index("section")
    q = lax.axis_index("seq")
    z = lax.axis_index("tensor")
    _, rows, width = states.shape
    chunks = x.shape[0]
    model = chunks * width
    part_rows = rows // tensors
    q_width = wq.shape[1]
    kv_width = wk.shape[1]
    q_heads = q_width // HEAD_DIM
    kv_heads = kv_width // HEAD_DIM
    group = q_heads // kv_heads
    span_count = order.shape[0]
    span = rows * seqs // span_count
    roles = 2

    def helper(s, r):
        return s + 1 - 2 * lax.rem(s, 2) if r == 0 else lax.rem(s + sections // 2, sections)

    def remote(src, dst, send, recv, device):
        return pltpu.make_async_remote_copy(
            src_ref=src, dst_ref=dst, send_sem=send, recv_sem=recv, device_id=device, device_id_type=MESH
        )

    right = {"tensor": lax.rem(z + 1, tensors)}
    left = {"tensor": lax.rem(z + tensors - 1, tensors)}

    loads = [
        pltpu.make_async_copy(src.at[0], dst, w_sem.at[i])
        for i, (src, dst) in enumerate(((wk_hbm, wk), (wv_hbm, wv), (wq_hbm, wq), (wo_hbm, wo)))
    ]
    for load in loads:
        load.start()

    barrier = pltpu.get_barrier_semaphore()
    for axis, here, count in (("tensor", z, tensors), ("seq", q, seqs), ("section", t, sections)):
        for step in range(1, count):
            pl.semaphore_signal(barrier, inc=1, device_id={axis: lax.rem(here + step, count)}, device_id_type=MESH)
    pl.semaphore_wait(barrier, tensors + seqs + sections - 3)

    def block(o):
        return pl.ds(pl.multiple_of(o * part_rows, part_rows), part_rows)

    def piece(s, c, o):
        first = 1 - lax.div(s + sections - 1, sections)
        return x.at[c + first * (o - c), block(o + first * (c - o))]

    def gather(cs, ref, recv, ready, arrived):
        for d in range(tensors):
            for c in cs:
                def step(o, go_right, go_left):
                    if go_right:
                        @pl.when(z < tensors - 1)
                        def _():
                            remote(ref(c, o), ref(c, o), x_right.at[c, o], recv.at[c, o], right).start()
                    if go_left:
                        @pl.when(z > 0)
                        def _():
                            remote(ref(c, o), ref(c, o), x_left.at[c, o], recv.at[c, o], left).start()

                if d == 0:
                    ready(c)
                    step(z, True, True)
                    arrived(z)
                else:
                    @pl.when(z >= d)
                    def _():
                        remote(ref(c, z - d), ref(c, z - d), x_right.at[c, z - d], recv.at[c, z - d], right).wait_recv()
                        step(z - d, True, False)
                        arrived(z - d)

                    @pl.when(z + d < tensors)
                    def _():
                        remote(ref(c, z + d), ref(c, z + d), x_left.at[c, z + d], recv.at[c, z + d], left).wait_recv()
                        step(z + d, False, True)
                        arrived(z + d)

    def chain_right(c, b, src):
        return remote(src, from_left.at[c, b], r_send.at[c, b], l_recv.at[c, b], right)

    def chain_left(c, b, src):
        return remote(src, from_right.at[c, b], l_send.at[c, b], r_recv.at[c, b], left)

    def chain(cs, mine):
        def rightward(c, far):
            @pl.when(jnp.logical_and(z == 0, far > 0))
            def _():
                chain_right(c, far, mine(c, far)).start()

            @pl.when(jnp.logical_and(z > 0, far > z))
            def _():
                chain_right(c, far, from_left.at[c, far]).wait_recv()
                from_left[c, far] = (from_left[c, far].astype(f32) + mine(c, far)[...].astype(f32)).astype(bf16)
                chain_right(c, far, from_left.at[c, far]).start()

        def leftward(c, k):
            @pl.when(jnp.logical_and(z == tensors - 1, k < tensors - 1))
            def _():
                chain_left(c, k, mine(c, k)).start()

            @pl.when(jnp.logical_and(z < tensors - 1, k < z))
            def _():
                chain_left(c, k, from_right.at[c, k]).wait_recv()
                from_right[c, k] = (from_right[c, k].astype(f32) + mine(c, k)[...].astype(f32)).astype(bf16)
                chain_left(c, k, from_right.at[c, k]).start()

        for k in range(tensors):
            @pl.when(z < tensors // 2)
            def _():
                for c in cs:
                    rightward(c, tensors - 1 - k)
                for c in cs:
                    leftward(c, k)

            @pl.when(z >= tensors // 2)
            def _():
                for c in cs:
                    leftward(c, k)
                for c in cs:
                    rightward(c, tensors - 1 - k)

    def chain_end(c, mine):
        total[c] = mine(c, z)[...].astype(f32)

        @pl.when(z > 0)
        def _():
            chain_right(c, z, from_left.at[c, z]).wait_recv()
            total[c] += from_left[c, z].astype(f32)

        @pl.when(z < tensors - 1)
        def _():
            chain_left(c, z, from_right.at[c, z]).wait_recv()
            total[c] += from_right[c, z].astype(f32)

    def relay_ref(c, o):
        return relay.at[c, o]

    def deliver(s, r, o):
        return remote(relay.at[r, o], piece(s, r, o), deliver_send.at[r, o], x_recv.at[r, o], {"section": s})

    def onward_relay(r):
        goal = lax.rem(t + 1, sections)
        return remote(fresh.at[r], relay.at[r, z], next_send.at[r], relay_recv.at[r, z], {"section": helper(goal, r)})

    def onward(c):
        goal = lax.rem(t + 1, sections)
        return remote(fresh.at[c], x.at[c, block(z)], next_send.at[c], x_recv.at[c, z], {"section": goal})

    def raw_copy(r, b):
        return remote(
            part.at[r, block(b)], raw.at[r, block(b)], raw_send.at[r, b], raw_recv.at[r, b], {"section": helper(t, r)}
        )

    def back_copy(r):
        return remote(relay.at[roles + r, 0], back.at[r], back_send.at[r], back_recv.at[r], {"section": helper(t, r)})

    def raw_block(c, b):
        raw_copy(c, b).wait_recv()
        return raw.at[c, block(b)]

    def help_gather(s, r):
        def ready(c):
            @pl.when(s == 0)
            def _():
                relay[r, z] = states[0, r * part_rows:(r + 1) * part_rows, :]

            @pl.when(jnp.logical_and(s > 0, s == t + 1))
            def _():
                relay[r, z] = fresh[r]

            @pl.when(jnp.logical_and(s > 0, s != t + 1))
            def _():
                onward_relay(r).wait_recv()

        gather([r], relay_ref, relay_recv, ready, lambda o: deliver(s, r, o).start())

    def help_reduce(r):
        chain([r], raw_block)
        chain_end(r, raw_block)
        relay[roles + r, 0] = total[r].astype(bf16)
        back_copy(r).start()

    half = HEAD_DIM // 2

    def positions():
        row = lax.broadcasted_iota(jnp.int32, (rows, HEAD_DIM), 0) + q * rows
        starts = jnp.zeros((rows, HEAD_DIM), jnp.int32)
        key_col = lax.broadcasted_iota(jnp.int32, (1, rows * seqs), 1)
        key_starts = jnp.zeros((1, rows * seqs), jnp.int32)
        for j in range(span_count):
            begin = order[j] * span
            starts = jnp.where(row // span == j, begin, starts)
            key_starts = jnp.where(key_col // span == j, begin, key_starts)
        return starts + row % span, key_starts + key_col % span

    def rope(u):
        return u * cos_ref[...] + pltpu.roll(u, half, 1) * sin_ref[...]

    def tables():
        places, _ = positions()
        lane = lax.broadcasted_iota(jnp.int32, (rows, HEAD_DIM), 1)
        inverse = jnp.exp((lane % half).astype(f32) * (-2.0 / HEAD_DIM * math.log(rotary_base)))
        angles = places.astype(f32) * inverse
        cos_ref[...] = jnp.cos(angles)
        sin_ref[...] = jnp.sin(angles) * jnp.where(lane < half, -1.0, 1.0)

    def kv_copy(j, device):
        return remote(kv.at[j], kv.at[j], kv_send.at[device], kv_recv.at[j], {"seq": device})

    def share(c):
        return remote(fresh.at[c], landed.at[block(z)], out_send.at[c], out_recv.at[z], {"tensor": c})

    def part_block(c, b):
        return part.at[c, block(b)]

    def layer():
        line = list(range(roles, chunks))

        def own_piece(c, o):
            return piece(t, c, o)

        def ready(c):
            @pl.when(t > 0)
            def _():
                onward(c).wait_recv()

        gather(line, own_piece, x_recv, ready, lambda o: None)

        def delivered(r):
            for o in range(tensors):
                deliver(t, r, o).wait_recv()

        @pl.when(t == 0)
        def _():
            for r in range(roles):
                delivered(r)

        acc_q[...] = jnp.zeros_like(acc_q)
        acc_kv[...] = jnp.zeros_like(acc_kv)
        for load in loads[:3]:
            load.wait()

        def take_chunk(c, squares):
            stream = x[c].astype(f32)
            squares = squares + jnp.sum(stream * stream, axis=1, keepdims=True)
            scaled = (stream * gain_in[c].astype(f32)).astype(bf16)
            depth = pl.ds(pl.multiple_of(c * width, width), width)
            acc_kv[:, :kv_width] += jnp.dot(scaled, wk[depth, :], preferred_element_type=f32)
            acc_kv[:, kv_width:] += jnp.dot(scaled, wv[depth, :], preferred_element_type=f32)
            acc_q[...] += jnp.dot(scaled, wq[depth, :], preferred_element_type=f32)
            return squares

        squares = lax.fori_loop(roles, chunks, take_chunk, jnp.zeros((rows, 1), f32))
        for r in range(roles):
            @pl.when(t > 0)
            def _():
                delivered(r)

        squares = lax.fori_loop(0, roles, take_chunk, squares)
        scale = lax.rsqrt(squares / model + epsilon)
        for k in range(kv_heads):
            cols = pl.ds(k * HEAD_DIM, HEAD_DIM)
            kv[q, :, cols] = rope(acc_kv[:, cols] * scale).astype(bf16)
        kv[q, :, kv_width:] = (acc_kv[:, kv_width:] * scale).astype(bf16)
        for step in range(1, seqs):
            kv_copy(q, lax.rem(q + step, seqs)).start()
        for h in range(q_heads):
            cols = pl.ds(h * HEAD_DIM, HEAD_DIM)
            qh[:, cols] = (rope(acc_q[:, cols] * scale) * query_scale).astype(bf16)
        for step in range(1, seqs):
            other = lax.rem(q + step, seqs)
            kv_copy(other, other).wait_recv()

        places, key_places = positions()
        dims = (((1,), (1,)), ((), ()))
        for h in range(q_heads):
            k = h // group
            cols = pl.ds(h * HEAD_DIM, HEAD_DIM)
            queries = qh[:, cols]
            numerator = jnp.zeros((rows, HEAD_DIM), f32)
            totals = jnp.zeros((rows, 1), f32)
            for j in range(seqs):
                keys = kv[j, :, k * HEAD_DIM:(k + 1) * HEAD_DIM]
                vals = kv[j, :, kv_width + k * HEAD_DIM:kv_width + (k + 1) * HEAD_DIM]
                scores = lax.dot_general(queries, keys, dims, preferred_element_type=f32)
                capped = softcap_limit * jnp.tanh(scores * (1.0 / softcap_limit))
                allowed = key_places[:, j * rows:(j + 1) * rows] <= places[:, :1]
                weight = jnp.where(allowed, jnp.exp(capped), 0.0)
                totals = totals + jnp.sum(weight, axis=1, keepdims=True)
                numerator = numerator + jnp.dot(weight.astype(bf16), vals, preferred_element_type=f32)
            att[:, cols] = (numerator / totals).astype(bf16)

        loads[3].wait()
        for c in range(chunks):
            part[c] = jnp.dot(
                att[...], wo[:, c * width:(c + 1) * width], preferred_element_type=f32
            ).astype(bf16)
            if c < roles:
                for k in range(tensors):
                    raw_copy(c, k // 2 if k % 2 else tensors - 1 - k // 2).start()
        chain(line, part_block)
        for c in line:
            chain_end(c, part_block)
        squares = jnp.zeros((part_rows, 1), f32)
        for r in range(roles):
            back_copy(r).wait_recv()
            total[r] = back[r].astype(f32)
        for c in range(chunks):
            squares = squares + jnp.sum(total[c] * total[c], axis=1, keepdims=True)
        scaling = lax.rsqrt(squares / model + epsilon)
        for c in range(chunks):
            fresh[c] = (x[c, block(z)].astype(f32) + total[c] * scaling * gain_out[c].astype(f32)).astype(bf16)
            if c < roles:
                @pl.when(jnp.logical_and(t < sections - 1, helper(lax.rem(t + 1, sections), c) != t))
                def _():
                    onward_relay(c).start()
            else:
                @pl.when(t < sections - 1)
                def _():
                    onward(c).start()
        for c in range(chunks):
            @pl.when(z != c)
            def _():
                share(c).start()

    @pl.when(t == 0)
    def _():
        x[z, roles * part_rows:, :] = states[0, roles * part_rows:, :]

    tables()

    def turn(s, carry):
        @pl.when(s == t)
        def _():
            layer()

        for r in range(roles):
            @pl.when(s == helper(t, r))
            def _():
                help_gather(s, r)
                help_reduce(r)
        return carry

    lax.fori_loop(0, sections, turn, 0)

    own = block(z)
    landed[own] = fresh[z]
    for o in range(tensors):
        @pl.when(z != o)
        def _():
            remote(fresh.at[o], landed.at[block(o)], out_send.at[o], out_recv.at[o], {"tensor": o}).wait_recv()
    out[0, 0] = landed[...]

    for c in range(chunks):
        if c < roles:
            @pl.when(jnp.logical_and(t < sections - 1, helper(lax.rem(t + 1, sections), c) != t))
            def _():
                onward_relay(c).wait_send()
            back_copy(c).wait_send()
            for o in range(tensors):
                deliver(helper(t, c), c, o).wait_send()
                raw_copy(c, o).wait_send()
        else:
            @pl.when(t < sections - 1)
            def _():
                onward(c).wait_send()

        @pl.when(z != c)
        def _():
            share(c).wait_send()

    for step in range(1, seqs):
        kv_copy(q, lax.rem(q + step, seqs)).wait_send()

    def drain(c, carry):
        for o in range(tensors):
            @pl.when(jnp.logical_and(z < tensors - 1, o <= z))
            def _():
                remote(relay.at[0, o], relay.at[0, o], x_right.at[c, o], x_recv.at[c, o], right).wait_send()

            @pl.when(jnp.logical_and(z > 0, o >= z))
            def _():
                remote(relay.at[0, o], relay.at[0, o], x_left.at[c, o], x_recv.at[c, o], left).wait_send()

            @pl.when(o > z)
            def _():
                chain_right(c, o, from_left.at[c, o]).wait_send()

            @pl.when(o < z)
            def _():
                chain_left(c, o, from_right.at[c, o]).wait_send()
        return carry

    lax.fori_loop(0, chunks, drain, 0)


def body(sections, seqs, tensors, states_in, span_order, pre_gain, w_query, w_key, w_value, w_out, post_gain):
    _, rows, width = states_in.shape
    model = pre_gain.shape[1]
    chunks = model // width
    part_rows = rows // tensors
    q_width, kv_width = w_query.shape[2], w_key.shape[2]
    vmem = pl.BlockSpec(memory_space=pltpu.VMEM)
    hbm = pl.BlockSpec(memory_space=pl.ANY)
    smem = pl.BlockSpec(memory_space=pltpu.SMEM)
    dma = pltpu.SemaphoreType.DMA
    grid2 = (chunks, tensors)
    return pl.pallas_call(
        functools.partial(kernel, sections, seqs, tensors),
        out_shape=jax.ShapeDtypeStruct((1, 1, rows, width), bf16),
        in_specs=[vmem, smem, vmem, hbm, hbm, hbm, hbm, vmem],
        out_specs=vmem,
        scratch_shapes=[
            pltpu.VMEM((model, q_width), bf16),
            pltpu.VMEM((model, kv_width), bf16),
            pltpu.VMEM((model, kv_width), bf16),
            pltpu.VMEM((q_width, model), bf16),
            pltpu.VMEM((chunks, rows, width), bf16),
            pltpu.VMEM((rows, q_width), f32),
            pltpu.VMEM((rows, 2 * kv_width), f32),
            pltpu.VMEM((seqs, rows, 2 * kv_width), bf16),
            pltpu.VMEM((rows, q_width), bf16),
            pltpu.VMEM((rows, q_width), bf16),
            pltpu.VMEM((chunks, rows, width), bf16),
            pltpu.VMEM((chunks, tensors, part_rows, width), bf16),
            pltpu.VMEM((chunks, tensors, part_rows, width), bf16),
            pltpu.VMEM((chunks, part_rows, width), f32),
            pltpu.VMEM((chunks, part_rows, width), bf16),
            pltpu.VMEM((rows, width), bf16),
            pltpu.VMEM((4, tensors, part_rows, width), bf16),
            pltpu.VMEM((2, rows, width), bf16),
            pltpu.VMEM((2, part_rows, width), bf16),
            pltpu.VMEM((rows, HEAD_DIM), f32),
            pltpu.VMEM((rows, HEAD_DIM), f32),
            dma((4,)),
            dma(grid2), dma(grid2), dma(grid2),
            dma((2, tensors)), dma((2, tensors)),
            dma((seqs,)), dma((seqs,)),
            dma(grid2), dma(grid2), dma(grid2), dma(grid2),
            dma((2, tensors)), dma((2, tensors)), dma((2,)), dma((2,)),
            dma((chunks,)), dma((tensors,)), dma((tensors,)),
        ],
        compiler_params=pltpu.CompilerParams(
            collective_id=0, has_side_effects=True, vmem_limit_bytes=60 * 1024 * 1024
        ),
    )(
        states_in, span_order, pre_gain.reshape(chunks, 1, width), w_query, w_key, w_value, w_out,
        post_gain.reshape(chunks, 1, width),
    )


def solution(mesh):
    in_specs = (
        P(None, "seq", "tensor"),
        P(),
        P("section", None),
        P("section", None, "tensor"),
        P("section", None, "tensor"),
        P("section", None, "tensor"),
        P("section", "tensor", None),
        P("section", None),
    )
    out_specs = P("section", None, "seq", "tensor")
    sizes = (mesh.shape["section"], mesh.shape["seq"], mesh.shape["tensor"])
    return jax.shard_map(
        functools.partial(body, *sizes), mesh=mesh, in_specs=in_specs, out_specs=out_specs, check_vma=False
    )
```
